512 devices in a mesh: lat: 128 (over z, y, core), chan: 4 (over x).
Axes of the slice: x: 4, y: 8, z: 8, core: 2. Of those that a mesh axis runs over, the one named last changes fastest.
Arguments:
- grid_in: bfloat16 [256, 384, 1024], P('chan', 'lat'), may hold values from -6 to 6
- quad_weights: float32 [384], P('lat'), may hold values from 0.5 to 2
- legendre: bfloat16 [384, 384, 384], P('lat'), as said below
- mixing: bfloat16 [2, 384, 256, 256], P(None, 'lat', 'chan'), may hold values from -0.375 to 0.375
Outputs:
- grid_out: bfloat16 [256, 384, 1024], P('chan', 'lat')
The draws below stay inside these ranges and needn't reach their ends.
Inputs may be any that keep to these rules, and one draw needn't show every extreme that they name: legendre[m, l, t] is zero wherever l < m.
All inputs are finite; a program needn't handle non-finite values.
Results may differ from the reference program's by a relative error of at most 0.0068.
Values may be sent and summed in bfloat16 or wider, within the bound.
A program may use at most 64 MiB of HBM per device.

```python
import math
import jax
import jax.numpy as jnp
from jax import lax

C = 256
NLAT = 384
NLON = 1024
M = 384
L = 384


def draw_legendre(key, part):
    values = jax.random.normal(key, (M, L, NLAT), jnp.float32)
    orders = jnp.arange(M, dtype=jnp.int32)[:, None, None]
    degrees = jnp.arange(L, dtype=jnp.int32)[None, :, None]
    values = jnp.where(degrees >= orders, values, 0.0) * NLAT ** (-0.5)
    return values.astype(jnp.bfloat16)


def spiked(array, own_key, source, target, parts, factor):
    def block_of(axis_at):
        return (jnp.arange(array.shape[axis_at]) // (array.shape[axis_at] // parts)).reshape((-1,) + (1,) * (array.ndim - 1 - axis_at))

    one_side = jax.random.permutation(own_key, parts)[block_of(target)]
    second = (block_of(target) + parts // 2) % parts
    return jnp.where((block_of(source) == one_side) | (block_of(source) == second), factor * array, array)


def levels(rng, dims, pieces, smallest, largest):
    gain = 1.0
    for dim, shards_of in pieces:
        heights = jax.random.uniform(jax.random.fold_in(jax.random.fold_in(rng, 6), dim), (shards_of,), jnp.float32, smallest / len(pieces), largest / len(pieces))
        gain = gain * jnp.repeat(jnp.exp(heights), dims[dim] // shards_of).reshape((-1,) + (1,) * (len(dims) - 1 - dim))
    return gain


def gaussian(stream_key, extent, scale, limit, split=(), held_as=jnp.bfloat16):
    factor_of = levels(stream_key, extent, split, -0.22, 0.18) if split else 1.0
    drawn = jax.random.normal(stream_key, extent, jnp.float32) * scale * factor_of
    return jnp.minimum(jnp.maximum(drawn, -limit), limit).astype(held_as)


def noise_with(own_key, extent, scale, reach, cuts, heavy, kind=jnp.bfloat16):
    array = scale * jax.random.normal(own_key, extent, jnp.float32)
    if cuts:
        array = array * levels(own_key, extent, cuts, -0.22, 0.18)
    return jnp.clip(spiked(array, jax.random.fold_in(own_key, 3), *heavy), -reach, reach).astype(kind)


def setup_inputs(seed: int = 0) -> dict:
    arg_keys = jax.random.split(jax.random.key(seed), 5)
    grid_in = gaussian(arg_keys[0], (C, NLAT, NLON), 1.0, 6.0, ((0, 4), (1, 128)))
    quad_weights = jnp.clip(jnp.exp(math.log(2.0) - 1.3862944 * jax.random.uniform(arg_keys[1], (NLAT,), jnp.float32) ** levels(arg_keys[1], (NLAT,), ((0, 128),), -0.2, 0.2)), 0.5, 2.0)
    legendre = draw_legendre(jax.random.fold_in(arg_keys[4], 71), 0)
    mixing = noise_with(arg_keys[3], (2, L, C, C), (2 * C) ** -0.5, 0.375, ((1, 128), (2, 4)), (2, 3, 4, 2.0))
    return {"grid_in": grid_in, "quad_weights": quad_weights, "legendre": legendre, "mixing": mixing}


def fourier_table(number, length):
    orders = jnp.arange(number, dtype=jnp.int32)
    points = jnp.arange(length, dtype=jnp.int32)
    phases = orders[:, None] * points[None, :] % length
    angles = phases.astype(jnp.float32) * (2.0 * math.pi / length)
    factor = 1.0 / math.sqrt(length)
    return jnp.stack([jnp.cos(angles) * factor, -jnp.sin(angles) * factor]).astype(jnp.bfloat16)

def reference(grid_in, quad_weights, legendre, mixing):
    fourier = fourier_table(M, NLON)
    flattened = grid_in.reshape(C * NLAT, NLON)
    spectra = jnp.dot(flattened, fourier.reshape(2 * M, NLON).T, preferred_element_type=jnp.float32)
    spectra = spectra.reshape(C, NLAT, 2, M) * quad_weights[None, :, None, None]
    weighted = spectra.astype(jnp.bfloat16).transpose(3, 1, 2, 0).reshape(M, NLAT, 2 * C)

    def forward_one(operands):
        return jnp.dot(operands[0], operands[1], preferred_element_type=jnp.float32).astype(jnp.bfloat16)
    coeffs = lax.map(forward_one, (legendre, weighted))
    by_degree = coeffs.transpose(1, 0, 2)
    weights_by = mixing.transpose(1, 0, 2, 3)

    def mix_one(operands):
        values, weight = operands
        real_in = values[:, :C]
        imag_in = values[:, C:]
        real_out = jnp.dot(real_in, weight[0], preferred_element_type=jnp.float32) - jnp.dot(imag_in, weight[1], preferred_element_type=jnp.float32)
        imag_out = jnp.dot(imag_in, weight[0], preferred_element_type=jnp.float32) + jnp.dot(real_in, weight[1], preferred_element_type=jnp.float32)
        return jnp.concatenate([real_out, imag_out], axis=1).astype(jnp.bfloat16)
    mixed_coef = lax.map(mix_one, (by_degree, weights_by)).transpose(1, 0, 2)

    def inverse_one(operands):
        return jnp.dot(operands[0].T, operands[1], preferred_element_type=jnp.float32).astype(jnp.bfloat16)
    synthesis = lax.map(inverse_one, (legendre, mixed_coef))
    spread = synthesis.reshape(M, NLAT, 2, C).transpose(3, 1, 2, 0).reshape(C * NLAT, 2 * M)
    restored = jnp.dot(spread, fourier.reshape(2 * M, NLON), preferred_element_type=jnp.float32)
    return (restored.reshape(C, NLAT, NLON) + grid_in.astype(jnp.float32)).astype(jnp.bfloat16)
```

```python
import functools

import jax
import jax.numpy as jnp
import numpy as np
from jax import lax
from jax.experimental import pallas as pl
from jax.experimental.pallas import tpu as pltpu
from jax.sharding import PartitionSpec as P

MESH = pl.DeviceIdType.MESH
BF = jnp.bfloat16
F32 = jnp.float32


def fourier_rows(peers, length):
    slot = np.arange(2 * peers)
    near, far = 3 * (slot // 2) + slot % 2, 3 * (slot // 2) + 2
    points = np.arange(length)
    factor = np.float32(1.0 / np.sqrt(length))
    parts = []
    for orders in (near, far):
        phases = (orders[:, None] * points[None, :]) % length
        angles = phases.astype(np.float32) * np.float32(2.0 * np.pi / length)
        parts += [np.cos(angles) * factor, -np.sin(angles) * factor]
    return np.concatenate(parts).astype(BF)


def nt(a, b):
    return lax.dot_general(a, b, (((1,), (1,)), ((), ())), preferred_element_type=F32)


def nn(a, b):
    return jnp.dot(a, b, preferred_element_type=F32)


def kernel(
    peers, chans, grid_z, grid_y,
    x_hbm, quad, leg_hbm, mix_hbm, tab_hbm, out_hbm,
    x, leg, tab, picks, tables, turned, weights, mixer,
    send_a, got_a, send_b, got_b, send_c, got_c, send_d, got_d,
    spread_rows, total, result,
    load_sem, snd, rcv, w_snd, w_rcv,
):
    me, chan = lax.axis_index("lat"), lax.axis_index("chan")
    rows = 2 * peers
    width = x.shape[1]
    near, far = slice(0, 3), slice(3, 5)
    group = peers // chans
    pair_of = lambda p: pl.ds(2 * p, 2)
    stacked = lambda ref, part: ref[part].reshape(-1, 128)

    loads = [
        pltpu.make_async_copy(x_hbm, x, load_sem.at[0]),
        pltpu.make_async_copy(tab_hbm, tab, load_sem.at[1]),
        pltpu.make_async_copy(leg_hbm, leg, load_sem.at[2]),
        pltpu.make_async_copy(mix_hbm, weights.at[chan], load_sem.at[3]),
    ]
    for load in loads:
        load.start()

    core, y, z = lax.rem(me, 2), lax.rem(lax.div(me, 2), grid_y), lax.div(me, 2 * grid_y)

    def far_first(k, n):
        return lax.rem(n // 2 + (1 - 2 * lax.rem(k, 2)) * lax.div(k + 1, 2), n)

    def peer_of(k):
        pz = lax.rem(z + far_first(lax.div(k, 2 * grid_y), grid_z), grid_z)
        py = lax.rem(y + far_first(lax.rem(lax.div(k, 2), grid_y), grid_y), grid_y)
        return (pz * grid_y + py) * 2 + lax.rem(core + 1 + lax.rem(k, 2), 2)

    barrier = pltpu.get_barrier_semaphore()

    @pl.loop(0, peers - 1)
    def _(k):
        pl.semaphore_signal(barrier, inc=1, device_id=(peer_of(k), chan), device_id_type=MESH)

    for d in range(1, chans):
        pl.semaphore_signal(barrier, inc=1, device_id=(me, lax.rem(chan + d, chans)), device_id_type=MESH)

    slot = lax.broadcasted_iota(jnp.int32, (rows, 3 * peers), 0)
    column = lax.broadcasted_iota(jnp.int32, (rows, 3 * peers), 1)
    base = 3 * (slot >> 1)
    odd = (slot & 1) == 1
    one = lambda mask: jnp.where(mask, 1.0, 0.0).astype(BF)
    for u in range(3):
        hit = column == base + u
        picks[0, u * rows : (u + 1) * rows] = one(hit & jnp.logical_not(odd))
        picks[1, u * rows : (u + 1) * rows] = one(hit & odd)
    picks[2, 0:rows] = one(column == base + (slot & 1))
    picks[2, rows : 2 * rows] = one((column == base + 2) & jnp.logical_not(odd))

    loads[0].wait()
    loads[1].wait()
    points = x[...].reshape(3 * width, x.shape[2])
    odd_row = (lax.broadcasted_iota(jnp.int32, (rows, 128), 0) & 1) == 1

    def waves(part):
        real = nt(tab[2 * part * rows : (2 * part + 1) * rows], points)
        imag = nt(tab[(2 * part + 1) * rows : (2 * part + 2) * rows], points)
        return [
            jnp.concatenate(
                [real[:, u * width : (u + 1) * width], imag[:, u * width : (u + 1) * width]], axis=1
            )
            * quad[u]
            for u in range(3)
        ]

    for u, value in enumerate(waves(0)):
        send_a[u] = value.astype(BF)
    first, second, third = waves(1)
    send_a[3] = jnp.where(odd_row, second, first).astype(BF)
    send_a[4] = jnp.where(odd_row, 0.0, third).astype(BF)

    loads[3].wait()
    pl.semaphore_wait(barrier, peers - 1 + chans - 1)

    def send_lat(src, dst, which):
        for g, part in enumerate((near, far)):
            sem = 2 * which + g

            @pl.loop(0, peers - 1)
            def _(k):
                p = peer_of(k)
                pltpu.make_async_remote_copy(
                    src_ref=src.at[part, pair_of(p)], dst_ref=dst.at[part, pair_of(me)],
                    send_sem=snd.at[sem], recv_sem=rcv.at[sem],
                    device_id=(p, chan), device_id_type=MESH,
                ).start()

            pltpu.make_async_copy(src.at[part, pair_of(me)], dst.at[part, pair_of(me)], rcv.at[sem]).start()
            yield

    def forward(src_ref, dst_ref, sem, target_lat, target_chan):
        here = jnp.logical_and(target_lat == me, target_chan == chan)

        @pl.when(here)
        def _():
            pltpu.make_async_copy(src_ref, dst_ref, rcv.at[sem]).start()

        @pl.when(jnp.logical_not(here))
        def _():
            pltpu.make_async_remote_copy(
                src_ref=src_ref, dst_ref=dst_ref, send_sem=snd.at[sem], recv_sem=rcv.at[sem],
                device_id=(target_lat, target_chan), device_id_type=MESH,
            ).start()

    def arrived(dst, which, g):
        part = (near, far)[g]
        pltpu.make_async_copy(dst.at[part], dst.at[part], rcv.at[2 * which + g]).wait()

    for _ in send_lat(send_a, got_a, 0):
        pass
    for d in range(1, chans):
        pltpu.make_async_remote_copy(
            src_ref=weights.at[chan], dst_ref=weights.at[chan],
            send_sem=w_snd.at[d - 1], recv_sem=w_rcv.at[d - 1],
            device_id=(me, lax.rem(chan + d, chans)), device_id_type=MESH,
        ).start()

    loads[2].wait()
    for u in range(3):
        at = slice(u * rows, (u + 1) * rows)
        value = 0.0
        for h in range(2):
            picked = nn(picks[h, at], leg[h]).astype(BF)
            value = value + nt(picked, picks[h])
        tables[0, at] = value.astype(BF)
    for q in range(2):
        at = slice(q * rows, (q + 1) * rows)
        picked = nn(picks[2, at], leg[2]).astype(BF)
        tables[1, at, 0 : 2 * rows] = nt(picked, picks[2, 0 : 2 * rows]).astype(BF)

    def send_degrees(g):
        part = (near, far)[g]
        own = lax.div(me, chans)

        @pl.loop(0, peers)
        def _(k):
            p = peer_of(k)
            forward(send_b.at[part, pair_of(p)], got_b.at[part, chan, pair_of(own)], 2 + g, p, lax.rem(me + p, chans))

    arrived(got_a, 0, 0)
    send_b[near] = nn(tables[0], stacked(got_a, near)).astype(BF).reshape(3, rows, 128)
    send_degrees(0)
    arrived(got_a, 0, 1)
    few = slice(0, 2 * rows)
    send_b[far] = nn(tables[1, few, few], stacked(got_a, far)).astype(BF).reshape(2, rows, 128)
    send_degrees(1)

    for u in range(3):
        at = slice(u * rows, (u + 1) * rows)
        value = 0.0
        for h in range(2):
            picked = nt(picks[h, at], leg[h]).astype(BF)
            value = value + nt(picked, picks[h])
        turned[0, at] = value.astype(BF)
    for q in range(2):
        at = slice(q * rows, (q + 1) * rows)
        picked = nt(picks[2, at], leg[2]).astype(BF)
        turned[1, at, 0 : 2 * rows] = nt(picked, picks[2, 0 : 2 * rows]).astype(BF)

    for d in range(1, chans):
        source = lax.rem(chan + chans - d, chans)
        pltpu.make_async_copy(weights.at[source], weights.at[source], w_rcv.at[d - 1]).wait()
    for degree in range(3):
        for c in range(chans):
            real, imag = weights[c, 0, degree], weights[c, 1, degree]
            upper, lower = [], []
            for d in range(chans):
                cut = slice(d * width, (d + 1) * width)
                upper += [real[:, cut], imag[:, cut]]
                lower += [-imag[:, cut], real[:, cut]]
            top = c * 2 * width
            mixer[degree, top : top + width] = jnp.concatenate(upper, axis=1)
            mixer[degree, top + width : top + 2 * width] = jnp.concatenate(lower, axis=1)

    some = 2 * group

    def values_of(q):
        return jnp.concatenate([got_b[q, c] for c in range(chans)], axis=1)

    def put_mixed(q, value):
        for d in range(chans):
            send_c[q, d] = value[:, d * 128 : (d + 1) * 128].astype(BF)

    def send_orders(g):
        part = (near, far)[g]
        shift = lax.rem(chan + peers - lax.rem(me, chans), chans)
        own = lax.div(me, chans)

        @pl.loop(0, peers)
        def _(k):
            d = lax.rem(chan + 2 + lax.rem(k, chans), chans)
            turn = lax.rem(own + group // 2 + lax.div(k, chans), group)
            forward(send_c.at[part, d, pair_of(turn)], got_c.at[part, pair_of(me)], 4 + g, turn * chans + shift, d)

    arrived(got_b, 1, 0)
    for u in range(3):
        put_mixed(u, nn(values_of(u), mixer[u]))
    send_orders(0)
    arrived(got_b, 1, 1)
    both = values_of(3)
    odd_some = (lax.broadcasted_iota(jnp.int32, (some, chans * 128), 0) & 1) == 1
    put_mixed(3, jnp.where(odd_some, nn(both, mixer[1]), nn(both, mixer[0])))
    put_mixed(4, nn(values_of(4), mixer[2]))
    send_orders(1)

    back = send_lat(send_d, got_d, 3)
    arrived(got_c, 2, 0)
    send_d[near] = nn(turned[0], stacked(got_c, near)).astype(BF).reshape(3, rows, 128)
    next(back)
    arrived(got_c, 2, 1)
    send_d[far] = nn(turned[1, few, few], stacked(got_c, far)).astype(BF).reshape(2, rows, 128)
    next(back)

    odd_lane = (lax.broadcasted_iota(jnp.int32, (128, rows), 1) & 1) == 1
    arrived(got_d, 3, 0)
    for u in range(3):
        at = slice(u * width, (u + 1) * width)
        flipped = got_d[u].T
        spread_rows[at, 0:rows] = flipped[0:width]
        spread_rows[at, rows : 2 * rows] = flipped[width : 2 * width]
    total[...] = points.astype(F32) + nn(spread_rows[:, 0 : 2 * rows], tab[0 : 2 * rows])
    arrived(got_d, 3, 1)
    pair = got_d[3].T
    zero = jnp.zeros_like(pair)
    last = got_d[4].T
    for u, value in enumerate((jnp.where(odd_lane, zero, pair), jnp.where(odd_lane, pair, zero), jnp.where(odd_lane, zero, last))):
        at = slice(u * width, (u + 1) * width)
        spread_rows[at, 2 * rows : 3 * rows] = value[0:width]
        spread_rows[at, 3 * rows : 4 * rows] = value[width : 2 * width]
    done = total[...] + nn(spread_rows[:, 2 * rows : 4 * rows], tab[2 * rows : 4 * rows])
    result[...] = done.astype(BF).reshape(result.shape)
    store = pltpu.make_async_copy(result, out_hbm, load_sem.at[4])
    store.start()

    own_target = lax.rem(2 * me, chans) == chan
    for which, buffer in ((0, send_a), (1, send_a), (2, send_a), (3, send_a)):
        for g, part in enumerate((near, far)):
            sem = snd.at[2 * which + g]
            sent = buffer.at[part, pl.ds(0, rows - 2)]
            pltpu.make_async_copy(sent, sent, sem).wait()
            if which in (1, 2):
                extra = buffer.at[part, pl.ds(0, 2)]

                @pl.when(jnp.logical_not(own_target))
                def _():
                    pltpu.make_async_copy(extra, extra, sem).wait()

    for d in range(1, chans):
        pltpu.make_async_copy(weights.at[chan], weights.at[chan], w_snd.at[d - 1]).wait()
    store.wait()


def body(peers, chans, grid_z, grid_y, grid_in, quad_weights, legendre, mixing):
    width, _, length = grid_in.shape
    rows = 2 * peers
    table = jnp.asarray(fourier_rows(peers, length))
    plain = pltpu.VMEM((5, rows, 128), BF)
    split = pltpu.VMEM((5, chans, rows // chans, 128), BF)
    anywhere = pl.BlockSpec(memory_space=pl.ANY)
    dma = pltpu.SemaphoreType.DMA
    out = pl.pallas_call(
        functools.partial(kernel, peers, chans, grid_z, grid_y),
        out_shape=jax.ShapeDtypeStruct((3, width, length), BF),
        in_specs=[anywhere, pl.BlockSpec(memory_space=pltpu.SMEM), anywhere, anywhere, anywhere],
        out_specs=anywhere,
        scratch_shapes=[
            pltpu.VMEM((3, width, length), BF),
            pltpu.VMEM(legendre.shape, BF),
            pltpu.VMEM((4 * rows, length), BF),
            pltpu.VMEM((3, 3 * rows, 3 * peers), BF),
            pltpu.VMEM((2, 3 * rows, 3 * rows), BF),
            pltpu.VMEM((2, 3 * rows, 3 * rows), BF),
            pltpu.VMEM((chans, *mixing.shape), BF),
            pltpu.VMEM((3, chans * 2 * width, chans * 2 * width), BF),
            plain, plain, plain, split, split, plain, plain, plain,
            pltpu.VMEM((3 * width, 4 * rows), BF),
            pltpu.VMEM((3 * width, length), F32),
            pltpu.VMEM((3, width, length), BF),
            dma((5,)), dma((8,)), dma((8,)), dma((chans - 1,)), dma((chans - 1,)),
        ],
        compiler_params=pltpu.CompilerParams(
            collective_id=0, has_side_effects=True, vmem_limit_bytes=48 * 1024 * 1024
        ),
    )(grid_in.transpose(1, 0, 2), quad_weights, legendre, mixing, table)
    return out.transpose(1, 0, 2)


def solution(mesh):
    peers, chans = mesh.shape["lat"], mesh.shape["chan"]
    grid_y = grid_z = int(round((peers // 2) ** 0.5))
    return jax.shard_map(
        functools.partial(body, peers, chans, grid_z, grid_y),
        mesh=mesh,
        in_specs=(P("chan", "lat", None), P("lat"), P("lat", None, None), P(None, "lat", "chan", None)),
        out_specs=P("chan", "lat", None),
        check_vma=False,
    )
```

```python
import functools

import jax
import jax.numpy as jnp
import numpy as np
from jax import lax
from jax.experimental import pallas as pl
from jax.experimental.pallas import tpu as pltpu
from jax.sharding import PartitionSpec as P

MESH = pl.DeviceIdType.MESH
BF = jnp.bfloat16
F32 = jnp.float32


def fourier_rows(peers, length):
    slot = np.arange(2 * peers)
    near, far = 3 * (slot // 2) + slot % 2, 3 * (slot // 2) + 2
    points = np.arange(length)
    factor = np.float32(1.0 / np.sqrt(length))
    parts = []
    for orders in (near, far):
        phases = (orders[:, None] * points[None, :]) % length
        angles = phases.astype(np.float32) * np.float32(2.0 * np.pi / length)
        parts += [np.cos(angles) * factor, -np.sin(angles) * factor]
    return np.concatenate(parts).astype(BF)


def nt(a, b):
    return lax.dot_general(a, b, (((1,), (1,)), ((), ())), preferred_element_type=F32)


def nn(a, b):
    return jnp.dot(a, b, preferred_element_type=F32)


def kernel(
    peers, chans,
    x_hbm, quad, leg_hbm, mix_hbm, tab_hbm, result,
    x, leg, tab, picks, tables, turned, weights, mixer,
    send_a, got_a, send_b, got_b, send_c, got_c, send_d, got_d,
    spread_rows, total,
    load_sem, snd, rcv, w_snd, w_rcv,
):
    me, chan = lax.axis_index("lat"), lax.axis_index("chan")
    rows = 2 * peers
    width = x.shape[1]
    near, far = slice(0, 3), slice(3, 5)
    group = peers // chans
    pair_of = lambda p: pl.ds(2 * p, 2)
    stacked = lambda ref, part: ref[part].reshape(-1, 128)

    loads = [
        pltpu.make_async_copy(x_hbm, x, load_sem.at[0]),
        pltpu.make_async_copy(tab_hbm, tab, load_sem.at[1]),
        pltpu.make_async_copy(leg_hbm, leg, load_sem.at[2]),
        pltpu.make_async_copy(mix_hbm, weights.at[chan], load_sem.at[3]),
    ]
    for load in loads:
        load.start()

    def wrap(value, n):
        return jnp.where(value >= n, value - n, value)

    barrier = pltpu.get_barrier_semaphore()

    @pl.loop(1, peers, unroll=4)
    def _(k):
        pl.semaphore_signal(barrier, inc=1, device_id=(wrap(me + k, peers), chan), device_id_type=MESH)

    for d in range(1, chans):
        pl.semaphore_signal(barrier, inc=1, device_id=(me, lax.rem(chan + d, chans)), device_id_type=MESH)

    slot = lax.broadcasted_iota(jnp.int32, (rows, 3 * peers), 0)
    column = lax.broadcasted_iota(jnp.int32, (rows, 3 * peers), 1)
    base = 3 * (slot >> 1)
    odd = (slot & 1) == 1
    one = lambda mask: jnp.where(mask, 1.0, 0.0).astype(BF)
    for u in range(3):
        hit = column == base + u
        picks[0, u * rows : (u + 1) * rows] = one(hit & jnp.logical_not(odd))
        picks[1, u * rows : (u + 1) * rows] = one(hit & odd)
    picks[2, 0:rows] = one(column == base + (slot & 1))
    picks[2, rows : 2 * rows] = one((column == base + 2) & jnp.logical_not(odd))

    loads[0].wait()
    loads[1].wait()
    points = x[...].reshape(3 * width, x.shape[2])
    odd_row = (lax.broadcasted_iota(jnp.int32, (rows, 128), 0) & 1) == 1

    def waves(part):
        real = nt(tab[2 * part * rows : (2 * part + 1) * rows], points)
        imag = nt(tab[(2 * part + 1) * rows : (2 * part + 2) * rows], points)
        return [
            jnp.concatenate(
                [real[:, u * width : (u + 1) * width], imag[:, u * width : (u + 1) * width]], axis=1
            )
            * quad[u]
            for u in range(3)
        ]

    for u, value in enumerate(waves(0)):
        send_a[u] = value.astype(BF)
    first, second, third = waves(1)
    send_a[3] = jnp.where(odd_row, second, first).astype(BF)
    send_a[4] = jnp.where(odd_row, 0.0, third).astype(BF)

    loads[3].wait()
    pl.semaphore_wait(barrier, peers - 1 + chans - 1)

    def send_lat(src, dst, which):
        for g, part in enumerate((near, far)):
            sem = 2 * which + g

            @pl.loop(1, peers, unroll=4)
            def _(k):
                p = wrap(me + k, peers)
                pltpu.make_async_remote_copy(
                    src_ref=src.at[part, pair_of(p)], dst_ref=dst.at[part, pair_of(me)],
                    send_sem=snd.at[sem], recv_sem=rcv.at[sem],
                    device_id=(p, chan), device_id_type=MESH,
                ).start()

            pltpu.make_async_copy(src.at[part, pair_of(me)], dst.at[part, pair_of(me)], rcv.at[sem]).start()
            yield

    def forward(src_ref, dst_ref, sem, target_lat, target_chan):
        pltpu.make_async_remote_copy(
            src_ref=src_ref, dst_ref=dst_ref, send_sem=snd.at[sem], recv_sem=rcv.at[sem],
            device_id=(target_lat, target_chan), device_id_type=MESH,
        ).start()

    def forward_near(src_ref, dst_ref, sem, target_lat, target_chan):
        here = jnp.logical_and(target_lat == me, target_chan == chan)

        @pl.when(here)
        def _():
            pltpu.make_async_copy(src_ref, dst_ref, rcv.at[sem]).start()

        @pl.when(jnp.logical_not(here))
        def _():
            forward(src_ref, dst_ref, sem, target_lat, target_chan)

    def arrived(dst, which, g):
        part = (near, far)[g]
        pltpu.make_async_copy(dst.at[part], dst.at[part], rcv.at[2 * which + g]).wait()

    for _ in send_lat(send_a, got_a, 0):
        pass
    for d in range(1, chans):
        pltpu.make_async_remote_copy(
            src_ref=weights.at[chan], dst_ref=weights.at[chan],
            send_sem=w_snd.at[d - 1], recv_sem=w_rcv.at[d - 1],
            device_id=(me, lax.rem(chan + d, chans)), device_id_type=MESH,
        ).start()

    loads[2].wait()
    for u in range(3):
        at = slice(u * rows, (u + 1) * rows)
        value = 0.0
        for h in range(2):
            picked = nn(picks[h, at], leg[h]).astype(BF)
            value = value + nt(picked, picks[h])
        tables[0, at] = value.astype(BF)
    for q in range(2):
        at = slice(q * rows, (q + 1) * rows)
        picked = nn(picks[2, at], leg[2]).astype(BF)
        tables[1, at, 0 : 2 * rows] = nt(picked, picks[2, 0 : 2 * rows]).astype(BF)

    def send_degrees(g):
        part = (near, far)[g]
        landing = got_b.at[part, chan, pair_of(lax.div(me, chans))]
        meets = [lax.rem(2 * me + r, chans) for r in range(chans)]

        def one(how, k, r):
            p = wrap(me + k, peers)
            how(send_b.at[part, pair_of(p)], landing, 2 + g, p, meets[r])

        @pl.loop(1, peers // chans)
        def _(k):
            for r in range(chans):
                one(forward, k * chans + r, r)

        for r in range(chans):
            one(forward if r else forward_near, r, r)

    arrived(got_a, 0, 0)
    send_b[near] = nn(tables[0], stacked(got_a, near)).astype(BF).reshape(3, rows, 128)
    send_degrees(0)
    arrived(got_a, 0, 1)
    few = slice(0, 2 * rows)
    send_b[far] = nn(tables[1, few, few], stacked(got_a, far)).astype(BF).reshape(2, rows, 128)
    send_degrees(1)

    for u in range(3):
        at = slice(u * rows, (u + 1) * rows)
        value = 0.0
        for h in range(2):
            picked = nt(picks[h, at], leg[h]).astype(BF)
            value = value + nt(picked, picks[h])
        turned[0, at] = value.astype(BF)
    for q in range(2):
        at = slice(q * rows, (q + 1) * rows)
        picked = nt(picks[2, at], leg[2]).astype(BF)
        turned[1, at, 0 : 2 * rows] = nt(picked, picks[2, 0 : 2 * rows]).astype(BF)

    for d in range(1, chans):
        source = lax.rem(chan + chans - d, chans)
        pltpu.make_async_copy(weights.at[source], weights.at[source], w_rcv.at[d - 1]).wait()
    for degree in range(3):
        for c in range(chans):
            real, imag = weights[c, 0, degree], weights[c, 1, degree]
            upper, lower = [], []
            for d in range(chans):
                cut = slice(d * width, (d + 1) * width)
                upper += [real[:, cut], imag[:, cut]]
                lower += [-imag[:, cut], real[:, cut]]
            top = c * 2 * width
            mixer[degree, top : top + width] = jnp.concatenate(upper, axis=1)
            mixer[degree, top + width : top + 2 * width] = jnp.concatenate(lower, axis=1)

    some = 2 * group

    def values_of(q):
        return jnp.concatenate([got_b[q, c] for c in range(chans)], axis=1)

    def put_mixed(q, value):
        for d in range(chans):
            send_c[q, d] = value[:, d * 128 : (d + 1) * 128].astype(BF)

    def send_orders(g):
        part = (near, far)[g]
        shift = lax.rem(chan + peers - lax.rem(me, chans), chans)
        own = lax.div(me, chans)

        landing = got_c.at[part, pair_of(me)]

        def one(how, k):
            turn = wrap(own + k, group)
            for d in range(chans):
                how(send_c.at[part, d, pair_of(turn)], landing, 4 + g, turn * chans + shift, d)

        @pl.loop(1, group)
        def _(k):
            one(forward, k)

        one(forward_near, 0)

    arrived(got_b, 1, 0)
    for u in range(3):
        put_mixed(u, nn(values_of(u), mixer[u]))
    send_orders(0)
    arrived(got_b, 1, 1)
    both = values_of(3)
    odd_some = (lax.broadcasted_iota(jnp.int32, (some, chans * 128), 0) & 1) == 1
    put_mixed(3, jnp.where(odd_some, nn(both, mixer[1]), nn(both, mixer[0])))
    put_mixed(4, nn(values_of(4), mixer[2]))
    send_orders(1)

    back = send_lat(send_d, got_d, 3)
    arrived(got_c, 2, 0)
    send_d[near] = nn(turned[0], stacked(got_c, near)).astype(BF).reshape(3, rows, 128)
    next(back)
    arrived(got_c, 2, 1)
    send_d[far] = nn(turned[1, few, few], stacked(got_c, far)).astype(BF).reshape(2, rows, 128)
    next(back)

    odd_lane = (lax.broadcasted_iota(jnp.int32, (128, rows), 1) & 1) == 1
    arrived(got_d, 3, 0)
    for u in range(3):
        at = slice(u * width, (u + 1) * width)
        flipped = got_d[u].T
        spread_rows[at, 0:rows] = flipped[0:width]
        spread_rows[at, rows : 2 * rows] = flipped[width : 2 * width]
    total[...] = points.astype(F32) + nn(spread_rows[:, 0 : 2 * rows], tab[0 : 2 * rows])
    arrived(got_d, 3, 1)
    pair = got_d[3].T
    zero = jnp.zeros_like(pair)
    last = got_d[4].T
    for u, value in enumerate((jnp.where(odd_lane, zero, pair), jnp.where(odd_lane, pair, zero), jnp.where(odd_lane, zero, last))):
        at = slice(u * width, (u + 1) * width)
        spread_rows[at, 2 * rows : 3 * rows] = value[0:width]
        spread_rows[at, 3 * rows : 4 * rows] = value[width : 2 * width]
    done = total[...] + nn(spread_rows[:, 2 * rows : 4 * rows], tab[2 * rows : 4 * rows])
    result[...] = done.astype(BF).reshape(result.shape)

    own_target = lax.rem(2 * me, chans) == chan
    for which, buffer in ((0, send_a), (1, send_a), (2, send_a), (3, send_a)):
        for g, part in enumerate((near, far)):
            sem = snd.at[2 * which + g]
            sent = buffer.at[part, pl.ds(0, rows - 2)]
            pltpu.make_async_copy(sent, sent, sem).wait()
            if which in (1, 2):
                extra = buffer.at[part, pl.ds(0, 2)]

                @pl.when(jnp.logical_not(own_target))
                def _():
                    pltpu.make_async_copy(extra, extra, sem).wait()

    for d in range(1, chans):
        pltpu.make_async_copy(weights.at[chan], weights.at[chan], w_snd.at[d - 1]).wait()


def body(peers, chans, grid_in, quad_weights, legendre, mixing):
    width, _, length = grid_in.shape
    rows = 2 * peers
    table = jnp.asarray(fourier_rows(peers, length))
    plain = pltpu.VMEM((5, rows, 128), BF)
    split = pltpu.VMEM((5, chans, rows // chans, 128), BF)
    stay = pl.BlockSpec(memory_space=pltpu.HBM)
    dma = pltpu.SemaphoreType.DMA
    out = pl.pallas_call(
        functools.partial(kernel, peers, chans),
        out_shape=jax.ShapeDtypeStruct((3, width, length), BF),
        in_specs=[stay, pl.BlockSpec(memory_space=pltpu.SMEM), stay, stay, stay],
        out_specs=pl.BlockSpec(memory_space=pltpu.VMEM),
        scratch_shapes=[
            pltpu.VMEM((3, width, length), BF),
            pltpu.VMEM(legendre.shape, BF),
            pltpu.VMEM((4 * rows, length), BF),
            pltpu.VMEM((3, 3 * rows, 3 * peers), BF),
            pltpu.VMEM((2, 3 * rows, 3 * rows), BF),
            pltpu.VMEM((2, 3 * rows, 3 * rows), BF),
            pltpu.VMEM((chans, *mixing.shape), BF),
            pltpu.VMEM((3, chans * 2 * width, chans * 2 * width), BF),
            plain, plain, plain, split, split, plain, plain, plain,
            pltpu.VMEM((3 * width, 4 * rows), BF),
            pltpu.VMEM((3 * width, length), F32),
            dma((4,)), dma((8,)), dma((8,)), dma((chans - 1,)), dma((chans - 1,)),
        ],
        compiler_params=pltpu.CompilerParams(
            collective_id=0, has_side_effects=True, vmem_limit_bytes=67043328
        ),
    )(grid_in.transpose(1, 0, 2), quad_weights, legendre, mixing, table)
    return out.transpose(1, 0, 2)


def solution(mesh):
    peers, chans = mesh.shape["lat"], mesh.shape["chan"]
    return jax.shard_map(
        functools.partial(body, peers, chans),
        mesh=mesh,
        in_specs=(P("chan", "lat", None), P("lat"), P("lat", None, None), P(None, "lat", "chan", None)),
        out_specs=P("chan", "lat", None),
        check_vma=False,
    )
```
